32 devices in a mesh: section: 4 (over y, x), tensor: 2 (over core), dp: 4 (over z).
Axes of the slice: x: 2, y: 2, z: 4, core: 2. Of those that a mesh axis runs over, the one named last changes fastest.
Arguments:
- hidden_in: bfloat16 [128, 4096], P('dp', 'tensor'), may hold values from -6 to 6
- norm_gain: float32 [4, 4096], P('section'), may hold values from 0.25 to 1.75
- gate_weight: bfloat16 [4, 4096, 8192], P('section', 'dp', 'tensor'), may hold values from -0.09375 to 0.09375
- up_weight: bfloat16 [4, 4096, 8192], P('section', 'dp', 'tensor'), may hold values from -0.09375 to 0.09375
- down_weight: bfloat16 [4, 4096, 8192], P('section', 'dp', 'tensor'), may hold values from -0.0625 to 0.0625
- lengths: int32 [16], P('dp'), may hold values from 3 to 8
Outputs:
- rdm: float32 [4, 16, 16], P('section', 'dp')
The draws below stay inside these ranges and needn't reach their ends.
Inputs may be any that keep to these rules, and one draw needn't show every extreme that they name: `lengths`: the number of leading valid token rows of each sentence.
All inputs are finite; a program needn't handle non-finite values.
Results may differ from the reference program's by a relative error of at most 0.0012.
Values may be sent and summed in bfloat16 or wider, within the bound.
A program may use at most 192 MiB of HBM per device.

```python
import jax
import jax.numpy as jnp
from jax import lax

D = 4096
FF = 8192
LEN = 8
SENT = 16
TOKENS = 128
SECTIONS = 4
N_SECTION = 4


def plant(drawn, own_key, smallest, top_value):
    longest = drawn.shape.index(max(drawn.shape))
    spots = []
    for shift in (0, 1):
        where = [jax.random.randint(jax.random.fold_in(own_key, axis), (), 0, length) for axis, length in enumerate(drawn.shape)]
        where[longest] = (where[longest] + shift) % drawn.shape[longest]
        spots.append(tuple(where))
    return drawn.at[spots[0]].set(smallest).at[spots[1]].set(top_value)


def block_scale(own_key, shape, pieces, least, largest):
    loudness, own = 1.0, jax.random.fold_in(own_key, 6)
    for axis_at, parts in pieces:
        draws = jnp.exp(jax.random.uniform(jax.random.fold_in(own, axis_at), (parts,), jnp.float32, least / len(pieces), largest / len(pieces)))
        loudness = loudness * jnp.repeat(draws, shape[axis_at] // parts).reshape([-1 if axis == axis_at else 1 for axis in range(len(shape))])
    return loudness


def gaussian(stream_key, dims, deviation, most, split=(), kind=jnp.bfloat16):
    values = deviation * jax.random.normal(stream_key, dims, jnp.float32)
    if split:
        values = values * block_scale(stream_key, dims, split, -0.22, 0.18)
    return jnp.clip(values, -most, most).astype(kind)


def setup_inputs(seed: int = 0) -> dict:
    keys = jax.random.split(jax.random.key(seed), 7)
    return {
        "hidden_in": gaussian(keys[0], (TOKENS, D), 1.0, 6.0, ((0, 4), (1, 2))),
        "norm_gain": jnp.clip(1.0 + 0.15 * jax.random.normal(keys[1], (SECTIONS, D), jnp.float32), 0.25, 1.75),
        "gate_weight": gaussian(keys[2], (SECTIONS, D, FF), D ** -0.5, 0.09375, ((0, 4), (1, 4), (2, 2))),
        "up_weight": gaussian(keys[3], (SECTIONS, D, FF), D ** -0.5, 0.09375, ((0, 4), (1, 4), (2, 2))),
        "down_weight": gaussian(keys[4], (SECTIONS, D, FF), FF ** -0.5, 0.0625, ((0, 4), (1, 4), (2, 2))),
        "lengths": plant(jax.random.randint(keys[5], (SENT,), 3, LEN + 1), jax.random.fold_in(keys[5], 1), 3, LEN).astype(jnp.int32),
    }


RMS_EPS = 1e-05
UNIT_FLOOR = 0.1
CONTRACT_LAST = (((1,), (1,)), ((), ()))

def reference(hidden_in, norm_gain, gate_weight, up_weight, down_weight, lengths):
    current = hidden_in
    positions = jnp.arange(LEN, dtype=jnp.int32)
    weights = (positions[None, :] < lengths[:, None]).astype(jnp.float32)
    counts = lengths.astype(jnp.float32)
    results = []
    for layer in range(N_SECTION):
        wide_state = current.astype(jnp.float32)
        inv_rms = lax.rsqrt(lax.optimization_barrier(jnp.mean(wide_state * wide_state, axis=1, keepdims=True)) + RMS_EPS)
        normed = (wide_state * inv_rms * norm_gain[layer][None, :]).astype(jnp.bfloat16)
        gate_sum = jnp.dot(normed, gate_weight[layer], preferred_element_type=jnp.float32)
        up_sum = jnp.dot(normed, up_weight[layer], preferred_element_type=jnp.float32)
        hidden = (jax.nn.silu(gate_sum) * up_sum).astype(jnp.bfloat16)
        summed = lax.dot_general(hidden, down_weight[layer], CONTRACT_LAST, preferred_element_type=jnp.float32)
        current = (wide_state + summed).astype(jnp.bfloat16)
        shaped = current.astype(jnp.float32).reshape(SENT, LEN, D)
        pooled = lax.optimization_barrier(jnp.sum(shaped * weights[:, :, None], axis=1)) / counts[:, None]
        centered = pooled - lax.optimization_barrier(jnp.mean(pooled, axis=1, keepdims=True))
        unit_rows = (centered * lax.rsqrt(lax.optimization_barrier(jnp.mean(centered * centered, axis=1, keepdims=True)) + UNIT_FLOOR)).astype(jnp.bfloat16)
        products = lax.dot_general(unit_rows, unit_rows, CONTRACT_LAST, preferred_element_type=jnp.float32)
        results.append(1.0 - products / D)
    return jnp.stack(results)
```

```python
import functools

import jax
import jax.numpy as jnp
from jax import lax
from jax.experimental import pallas as pl
from jax.experimental.pallas import tpu as pltpu
from jax.sharding import PartitionSpec as P

RMS_EPS = 1e-05
UNIT_FLOOR = 0.1
CONTRACT_LAST = (((1,), (1,)), ((), ()))
MESH = pl.DeviceIdType.MESH
LANES = 128
F32 = jnp.float32
BF16 = jnp.bfloat16

SPLIT = 2
Q = 2
AHEAD = 2

LEAF = (("G", (0, 1, 2, 3), 0), ("F", ((0, 0), (1, 0), (0, 1), (1, 1)), 1), ("E", None, 2))
HUB = (("G", (0, 1), 0), ("A", 0, 1), ("G", (2, 3), 0), ("A", 1, 1), ("C", 0, 0), ("F", ((0, 0), (0, 1)), 1),
       ("C", 1, 0), ("F", ((1, 0), (1, 1)), 1), ("E", None, 2))


def kernel(dps, tensors, sections, hidden_ref, gain_ref, lens_ref, gate_hbm, up_hbm, down_hbm,
           out_ref, gate_v, up_v, down_v, x_in, x_parts, scaled_v, part_out, part_in, own_gu, own_ss, half_ss, inv_v,
           cross_out, cross_in, h_out, hid, acc_v, tx, outs, gram, lbuf, lens_full,
           w_sem, d_send, d_recv, x_send, x_recv, p_send, p_recv, r_send, r_recv, h_send, h_recv, t_send, t_recv,
           g_send, g_recv, l_send, l_recv):
    section = lax.axis_index("section")
    tensor = lax.axis_index("tensor")
    dp = lax.axis_index("dp")
    micros = dps * SPLIT
    width = gate_v.shape[0]
    cols = gate_v.shape[1]
    fc = cols // (2 * Q)
    rows = x_in.shape[1]
    d_model = width * dps
    half = dps // 2
    pair = 2 if tensors % 2 == 0 else 1
    lead = pair - 1
    first = tensor - lax.rem(tensor, pair)
    core = lax.rem(tensor, pair)
    side = dp // half
    hub_dp = half - 1 + side
    out_way = 2 * side - 1
    reach = (dp - hub_dp) * out_way
    is_hub = jnp.logical_and(reach == 0, core == lead)
    held = hidden_ref.shape[1]
    pw = min(held, width)
    nj = held // pw
    np_ = width // pw

    def chunk_at(which, q):
        return (side if which == 0 else 1 - side) * Q + q

    def chunk_of(j):
        return chunk_at(1, j) if j < Q else chunk_at(0, j - Q)

    def columns(c):
        return pl.ds(pl.multiple_of(c * fc, fc), fc)

    def wcopy(which, c):
        src, dst = ((gate_hbm, gate_v), (up_hbm, up_v), (down_hbm, down_v))[which]
        return pltpu.make_async_copy(src.at[0, :, columns(c)], dst.at[:, columns(c)], w_sem.at[which, c])

    for j in range(2 * Q):
        wcopy(0, chunk_of(j)).start()
        wcopy(1, chunk_of(j)).start()
    for which, q in [(w, q) for q in range(Q) for w in range(2)]:
        wcopy(2, chunk_at(which, q)).start()

    barrier = pltpu.get_barrier_semaphore()
    for kt in range(tensors):
        for kd in range(dps):
            if kt or kd:
                pl.semaphore_signal(
                    barrier, inc=1,
                    device_id={"tensor": lax.rem(tensor + kt, tensors), "dp": lax.rem(dp + kd, dps)},
                    device_id_type=MESH)

    @pl.when(section > 0)
    def _():
        for k in range(tensors):
            pl.semaphore_signal(barrier, inc=1, device_id={"section": section - 1, "tensor": k}, device_id_type=MESH)

    @pl.when(section < sections - 1)
    def _():
        for k in range(tensors):
            pl.semaphore_signal(barrier, inc=1, device_id={"section": section + 1, "tensor": k}, device_id_type=MESH)

    pl.semaphore_wait(
        barrier,
        tensors * dps - 1 + jnp.where(section == 0, 0, tensors) + jnp.where(section == sections - 1, 0, tensors))

    each = lens_ref.shape[0]
    sents = each * dps
    peers = [lax.rem(dp + k, dps) for k in range(1, dps)]
    slot = lax.broadcasted_iota(jnp.int32, lbuf.shape[1:], 0)
    own_lens = jnp.ones(lbuf.shape[1:], F32)
    for n in range(each):
        own_lens = jnp.where(slot == n, lens_ref[n].astype(F32), own_lens)
    lbuf[dp] = own_lens

    def s_copy(buf, send, recv, c, peer):
        return pltpu.make_async_remote_copy(
            src_ref=buf.at[c], dst_ref=buf.at[c], send_sem=send.at[peer], recv_sem=recv.at[c],
            device_id={"dp": peer}, device_id_type=MESH)

    def spread(m, j, k):
        h = lax.rem(m, SPLIT)
        at = tensor * held + j * pw
        piece = lax.rem(at, width) // pw
        return pltpu.make_async_remote_copy(
            src_ref=hidden_ref.at[pl.ds(pl.multiple_of(h * rows, rows), rows), pl.ds(j * pw, pw)],
            dst_ref=x_in.at[m, :, pl.ds(pl.multiple_of(piece * pw, pw), pw)],
            send_sem=d_send.at[h, j * tensors + k], recv_sem=d_recv.at[m, piece],
            device_id={"tensor": lax.rem(tensor + k, tensors), "dp": at // width}, device_id_type=MESH)

    def spread_all(m, act):
        @pl.when(jnp.logical_and(section == 0, m // SPLIT == dp))
        def _():
            for j in range(nj):
                at = tensor * held + j * pw
                for k in range(tensors):
                    if k:
                        act(m, j, k)
                    else:
                        @pl.when(at // width != dp)
                        def _():
                            act(m, j, k)

    def spread_start(m):
        spread_all(m, lambda m, j, k: spread(m, j, k).start())

        @pl.when(jnp.logical_and(section == 0, m // SPLIT == dp))
        def _():
            h = lax.rem(m, SPLIT)
            for j in range(nj):
                at = tensor * held + j * pw
                piece = lax.rem(at, width) // pw

                @pl.when(at // width == dp)
                def _():
                    x_in[m, :, pl.ds(pl.multiple_of(piece * pw, pw), pw)] = hidden_ref[
                        pl.ds(pl.multiple_of(h * rows, rows), rows), j * pw:(j + 1) * pw]

    def early(m, carry):
        spread_start(m)
        return carry

    lax.fori_loop(0, AHEAD, early, 0)
    for c in peers:
        s_copy(lbuf, l_send, l_recv, dp, c).start()

    def p_part(ref, j):
        return ref.at[:, pl.ds(0, 2 * fc + LANES)] if j == 0 else ref.at[:, pl.ds(0, 2 * fc)]

    def p_copy(m, j):
        at = reach * pair + core
        return pltpu.make_async_remote_copy(
            src_ref=p_part(part_out.at[m, j], j), dst_ref=p_part(part_in.at[m, at, j], j),
            send_sem=p_send.at[m, j], recv_sem=p_recv.at[m, at * 2 * Q + j],
            device_id={"dp": hub_dp, "tensor": first + lead}, device_id_type=MESH)

    def p_wait(m, at, j):
        ref = p_part(part_in.at[m, at, j], j)
        pltpu.make_async_remote_copy(
            src_ref=ref, dst_ref=ref, send_sem=p_send.at[m, j], recv_sem=p_recv.at[m, at * 2 * Q + j],
            device_id={"dp": 1 - side}, device_id_type=MESH).wait_recv()

    def r_copy(m, k, q):
        j = 0 if q == 0 and k == lead else 1
        return pltpu.make_async_remote_copy(
            src_ref=p_part(cross_out.at[m, k, q], j), dst_ref=p_part(cross_in.at[m, k, q], j),
            send_sem=r_send.at[m, k * Q + q], recv_sem=r_recv.at[m, k * Q + q],
            device_id={"dp": hub_dp - out_way}, device_id_type=MESH)

    targets = [dp - out_way * r for r in range(half, 0, -1)] + [dp + out_way * r for r in range(1, half)]

    def h_copy(m, k, q, n):
        to = {"dp": targets[n], "tensor": first + k} if n < dps - 1 else {"tensor": first + k}
        return pltpu.make_async_remote_copy(
            src_ref=h_out.at[m, k, q], dst_ref=hid.at[m, side * Q + q],
            send_sem=h_send.at[m, (k * Q + q) * dps + n], recv_sem=h_recv.at[m, side * Q + q],
            device_id=to, device_id_type=MESH)

    def h_wait(m, c):
        pltpu.make_async_remote_copy(
            src_ref=hid.at[m, c], dst_ref=hid.at[m, c], send_sem=h_send.at[m, 0], recv_sem=h_recv.at[m, c],
            device_id={"dp": 1 - side}, device_id_type=MESH).wait_recv()

    def h_sends(k):
        return range(dps - 1 if k == lead else dps)

    def t_copy(m, t, peer):
        return pltpu.make_async_remote_copy(
            src_ref=tx.at[m, t], dst_ref=tx.at[m, t],
            send_sem=t_send.at[m, peer], recv_sem=t_recv.at[m, t],
            device_id={"tensor": peer}, device_id_type=MESH)

    def x_copy(m, t, k, to):
        return pltpu.make_async_remote_copy(
            src_ref=tx.at[m, t], dst_ref=x_parts.at[m, t],
            send_sem=x_send.at[m, k], recv_sem=x_recv.at[m, t],
            device_id={"section": to, "tensor": k}, device_id_type=MESH)

    lane = lax.broadcasted_iota(jnp.int32, (rows, LANES), 1)

    def pack(ss):
        high = ss.astype(BF16)
        low = (ss - high.astype(F32)).astype(BF16)
        return jnp.where(lane < LANES // 2, high.astype(F32), low.astype(F32)).astype(BF16)

    def unpack(lanes):
        return jnp.sum(lanes.astype(F32), axis=1, keepdims=True) * (2.0 / LANES)

    def enter(m):
        @pl.when(section == 0)
        def _():
            for piece in range(np_):
                source = (dp * width + piece * pw) // held

                @pl.when(jnp.logical_not(jnp.logical_and(m // SPLIT == dp, source == tensor)))
                def _():
                    ref = x_in.at[m, :, pl.ds(piece * pw, pw)]
                    pltpu.make_async_remote_copy(
                        src_ref=ref, dst_ref=ref, send_sem=d_send.at[0, 0], recv_sem=d_recv.at[m, piece],
                        device_id={"dp": 1 - side}, device_id_type=MESH).wait_recv()

        @pl.when(section > 0)
        def _():
            total = None
            for t in range(tensors):
                x_copy(m, t, 0, 0).wait_recv()
                term = x_parts[m, t].astype(F32)
                total = term if total is None else total + term
            x_in[m] = total.astype(BF16)

        x = x_in[m].astype(F32)
        own_ss[m] = jnp.broadcast_to(jnp.sum(x * x, axis=1, keepdims=True), (rows, LANES))
        scaled_v[...] = (x * gain_ref[:, pl.ds(pl.multiple_of(dp * width, width), width)]).astype(BF16)

    def project(m, hub, js):
        if js[0] == 0:
            enter(m)
        for j in js:
            c = chunk_of(j)

            @pl.when(m == 0)
            def _():
                wcopy(0, c).wait()
                wcopy(1, c).wait()

            g = jnp.dot(scaled_v[...], gate_v[:, columns(c)], preferred_element_type=F32)
            u = jnp.dot(scaled_v[...], up_v[:, columns(c)], preferred_element_type=F32)
            if hub:
                own_gu[m, j, :, 0:fc] = g
                own_gu[m, j, :, fc:2 * fc] = u
            else:
                part_out[m, j, :, 0:fc] = g.astype(BF16)
                part_out[m, j, :, fc:2 * fc] = u.astype(BF16)
                if j == 0:
                    part_out[m, j, :, 2 * fc:2 * fc + LANES] = pack(own_ss[m][:, 0:1])
                p_copy(m, j).start()

    def sources(k):
        return [r * pair + k for r in range(half) if r or k != lead]

    def gathered(m, k, j):
        total = own_gu[m, j] if k == lead else None
        for at in sources(k):
            term = part_in[m, at, j, :, 0:2 * fc].astype(F32)
            total = term if total is None else total + term
        return total

    def combine(m, q):
        for k in reversed(range(pair)):
            for at in sources(k):
                p_wait(m, at, q)
            cross_out[m, k, q, :, 0:2 * fc] = gathered(m, k, q).astype(BF16)
            if q == 0 and k == lead:
                ss = own_ss[m][:, 0:1]
                for at in sources(k):
                    ss = ss + unpack(part_in[m, at, 0, :, 2 * fc:2 * fc + LANES])
                half_ss[m] = jnp.broadcast_to(ss, (rows, LANES))
                cross_out[m, k, q, :, 2 * fc:2 * fc + LANES] = pack(ss)
            r_copy(m, k, q).start()

    def activate(m, q):
        for k in reversed(range(pair)):
            for at in sources(k):
                p_wait(m, at, Q + q)
            r_copy(m, k, q).wait_recv()
            if q == 0 and k == lead:
                ss = half_ss[m][:, 0:1] + unpack(cross_in[m, k, 0, :, 2 * fc:2 * fc + LANES])
                inv_v[m] = jnp.broadcast_to(lax.rsqrt(ss * (1.0 / d_model) + RMS_EPS), (rows, LANES))
            gu = (gathered(m, k, Q + q) + cross_in[m, k, q, :, 0:2 * fc].astype(F32)) * inv_v[m][:, 0:1]
            g = gu[:, 0:fc]
            made = (g / (1.0 + jnp.exp(-g)) * gu[:, fc:2 * fc]).astype(BF16)
            h_out[m, k, q] = made
            for n in h_sends(k):
                h_copy(m, k, q, n).start()
            if k == lead:
                hid[m, side * Q + q] = made

    def descend(m, hub, parts):
        acc = None if parts[0] == (0, 0) else acc_v[m]
        for which, q in parts:
            c = chunk_at(which, q)
            if not (hub and which == 0):
                h_wait(m, c)

            @pl.when(m == 0)
            def _():
                wcopy(2, c).wait()

            term = lax.dot_general(hid[m, c], down_v[:, columns(c)], CONTRACT_LAST, preferred_element_type=F32)
            acc = term if acc is None else acc + term
        if parts[-1] != (1, Q - 1):
            acc_v[m] = acc
        else:
            tx[m, tensor] = (acc + x_in[m].astype(F32) * (1.0 / tensors)).astype(BF16)

            @pl.when(section < sections - 1)
            def _():
                for k in range(tensors):
                    x_copy(m, tensor, k, section + 1).start()

            for k in range(1, tensors):
                t_copy(m, tensor, lax.rem(tensor + k, tensors)).start()

    def settle(m):
        for k in range(1, tensors):
            other = lax.rem(tensor + k, tensors)
            t_copy(m, other, other).wait_recv()
        total = tx[m, 0].astype(F32)
        for t in range(1, tensors):
            total = total + tx[m, t].astype(F32)
        outs[m] = total.astype(BF16)

    def run(plan, hub):
        def step(i, carry):
            spread_next = i + AHEAD

            @pl.when(spread_next < micros)
            def _():
                spread_start(spread_next)

            for op, arg, lag in plan:
                m = i - lag

                @pl.when(jnp.logical_and(m >= 0, m < micros))
                def _():
                    if op == "G":
                        project(m, hub, arg)
                    elif op == "C":
                        combine(m, arg)
                    elif op == "A":
                        activate(m, arg)
                    elif op == "F":
                        descend(m, hub, arg)
                    else:
                        settle(m)
            return carry

        lax.fori_loop(0, micros + max(lag for _, _, lag in plan), step, 0)

    @pl.when(is_hub)
    def _():
        run(HUB, True)

        def drain(m, carry):
            for k in range(pair):
                for q in range(Q):
                    r_copy(m, k, q).wait_send()
                    for n in h_sends(k):
                        h_copy(m, k, q, n).wait_send()
            return carry

        lax.fori_loop(0, micros, drain, 0)

    @pl.when(jnp.logical_not(is_hub))
    def _():
        run(LEAF, False)

        def drain(m, carry):
            for j in range(2 * Q):
                p_copy(m, j).wait_send()
            return carry

        lax.fori_loop(0, micros, drain, 0)

    for c in peers:
        s_copy(lbuf, l_send, l_recv, c, c).wait_recv()
    for c in range(dps):
        lens_full[c * each:(c + 1) * each] = lbuf[c, 0:each]
    tokens = micros * rows
    per = tokens // sents
    place = lax.broadcasted_iota(jnp.int32, (sents, tokens), 1) - per * lax.broadcasted_iota(
        jnp.int32, (sents, tokens), 0)
    lens = lens_full[:, 0:1]
    valid = jnp.logical_and(place >= 0, place.astype(F32) < lens)
    mask = jnp.where(valid, 1.0, 0.0).astype(BF16)
    pooled = jnp.dot(mask, outs[...].reshape(tokens, width), preferred_element_type=F32) / lens

    def share(buf, send, recv):
        for c in peers:
            s_copy(buf, send, recv, dp, c).start()
        for c in peers:
            s_copy(buf, send, recv, c, c).wait_recv()

    mean = jnp.sum(pooled, axis=1, keepdims=True) * (1.0 / width)
    centered = pooled - mean
    narrow = centered.astype(BF16)
    sq = jnp.sum(centered * centered, axis=1, keepdims=True)
    gram[dp, 0] = jnp.zeros((sents, LANES), F32)
    gram[dp, 0, :, 0:sents] = lax.dot_general(narrow, narrow, CONTRACT_LAST, preferred_element_type=F32)
    gram[dp, 1] = jnp.broadcast_to(sq, (sents, LANES))
    gram[dp, 2] = jnp.broadcast_to(mean, (sents, LANES))
    share(gram, g_send, g_recv)
    products, sq, mean = gram[0, 0], gram[0, 1], gram[0, 2]
    for c in range(1, dps):
        products = products + gram[c, 0]
        sq = sq + gram[c, 1]
        mean = mean + gram[c, 2]
    mean = mean * (1.0 / dps)
    r_i = lax.broadcasted_iota(jnp.int32, (sents, LANES), 0)
    c_i = lax.broadcasted_iota(jnp.int32, (sents, LANES), 1)
    for c in range(dps):
        off = gram[c, 2] - mean
        off_row = jnp.sum(jnp.where(r_i == c_i, off, 0.0), axis=0, keepdims=True)
        products = products + off * off_row * float(width)
        sq = sq + off * off * float(width)
    scale = lax.rsqrt(sq * (1.0 / d_model) + UNIT_FLOOR)
    across = jnp.sum(jnp.where(r_i == c_i, scale, 0.0), axis=0, keepdims=True)
    whole = 1.0 - products * scale * across * (1.0 / d_model)
    for r in range(each):
        row = jnp.sum(jnp.where(r_i == dp * each + r, whole, 0.0), axis=0, keepdims=True)
        out_ref[0, r:r + 1, :] = row[:, 0:sents]

    def drain(m, carry):
        spread_all(m, lambda m, j, k: spread(m, j, k).wait_send())
        for k in range(1, tensors):
            t_copy(m, tensor, lax.rem(tensor + k, tensors)).wait_send()

        @pl.when(section < sections - 1)
        def _():
            for k in range(tensors):
                x_copy(m, tensor, k, section + 1).wait_send()
        return carry

    lax.fori_loop(0, micros, drain, 0)
    for c in peers:
        s_copy(lbuf, l_send, l_recv, dp, c).wait_send()
        s_copy(gram, g_send, g_recv, dp, c).wait_send()


def per_device(hidden_in, norm_gain, gate_weight, up_weight, down_weight, lengths):
    sections = lax.axis_size("section")
    tensors = lax.axis_size("tensor")
    dps = lax.axis_size("dp")
    _, width, cols = gate_weight.shape
    micros = dps * SPLIT
    rows = hidden_in.shape[0] // SPLIT
    fc = cols // (2 * Q)
    half = dps // 2
    pair = 2 if tensors % 2 == 0 else 1
    held = hidden_in.shape[1]
    pw = min(held, width)
    each = lengths.shape[0]
    sents = each * dps
    vm = pl.BlockSpec(memory_space=pltpu.VMEM)
    hbm = pl.BlockSpec(memory_space=pl.ANY)
    dma = pltpu.SemaphoreType.DMA
    smem = pl.BlockSpec(memory_space=pltpu.SMEM)
    return pl.pallas_call(
        functools.partial(kernel, dps, tensors, sections),
        out_shape=jax.ShapeDtypeStruct((1, each, sents), F32),
        in_specs=[vm] * 2 + [smem] + [hbm] * 3,
        out_specs=vm,
        scratch_shapes=[
            pltpu.VMEM((width, cols), BF16),
            pltpu.VMEM((width, cols), BF16),
            pltpu.VMEM((width, cols), BF16),
            pltpu.VMEM((micros, rows, width), BF16),
            pltpu.VMEM((micros, tensors, rows, width), BF16),
            pltpu.VMEM((rows, width), BF16),
            pltpu.VMEM((micros, 2 * Q, rows, 2 * fc + LANES), BF16),
            pltpu.VMEM((micros, half * pair, 2 * Q, rows, 2 * fc + LANES), BF16),
            pltpu.VMEM((micros, 2 * Q, rows, 2 * fc), F32),
            pltpu.VMEM((micros, rows, LANES), F32),
            pltpu.VMEM((micros, rows, LANES), F32),
            pltpu.VMEM((micros, rows, LANES), F32),
            pltpu.VMEM((micros, pair, Q, rows, 2 * fc + LANES), BF16),
            pltpu.VMEM((micros, pair, Q, rows, 2 * fc + LANES), BF16),
            pltpu.VMEM((micros, pair, Q, rows, fc), BF16),
            pltpu.VMEM((micros, 2 * Q, rows, fc), BF16),
            pltpu.VMEM((micros, rows, width), F32),
            pltpu.VMEM((micros, tensors, rows, width), BF16),
            pltpu.VMEM((micros, rows, width), BF16),
            pltpu.VMEM((dps, 3, sents, LANES), F32),
            pltpu.VMEM((dps, -(-each // 8) * 8, LANES), F32),
            pltpu.VMEM((sents, LANES), F32),
            dma((3, 2 * Q)),
            dma((SPLIT, held // pw * tensors)),
            dma((micros, width // pw)),
            dma((micros, tensors)),
            dma((micros, tensors)),
            dma((micros, 2 * Q)),
            dma((micros, half * pair * 2 * Q)),
            dma((micros, pair * Q)),
            dma((micros, pair * Q)),
            dma((micros, pair * Q * dps)),
            dma((micros, 2 * Q)),
            dma((micros, tensors)),
            dma((micros, tensors)),
            dma((dps,)),
            dma((dps,)),
            dma((dps,)),
            dma((dps,)),
        ],
        compiler_params=pltpu.CompilerParams(
            collective_id=0, has_side_effects=True, vmem_limit_bytes=60 * 1024 * 1024),
    )(hidden_in, norm_gain, lengths, gate_weight, up_weight, down_weight)


def solution(mesh):
    placed = (
        P("dp", "tensor"),
        P("section", None),
        P("section", "dp", "tensor"),
        P("section", "dp", "tensor"),
        P("section", "dp", "tensor"),
        P("dp"),
    )
    return jax.shard_map(
        per_device, mesh=mesh, in_specs=placed, out_specs=P("section", "dp", None), check_vma=False
    )
```

```python
import functools

import jax
import jax.numpy as jnp
from jax import lax
from jax.experimental import pallas as pl
from jax.experimental.pallas import tpu as pltpu
from jax.sharding import PartitionSpec as P

RMS_EPS = 1e-05
UNIT_FLOOR = 0.1
CONTRACT_LAST = (((1,), (1,)), ((), ()))
MESH = pl.DeviceIdType.MESH
LANES = 128
F32 = jnp.float32
BF16 = jnp.bfloat16

SPLIT = 2
Q = 2
AHEAD = 8

LEAF = (("G", (0, 1), 0), ("F", ((0, 1), (1, 1)), 2), ("E", None, 3), ("G", (2, 3), 0), ("F", ((0, 0), (1, 0)), 1))
HUB = (("G", (0, 1), 0), ("F", ((1, 0), (1, 1)), 2), ("E", None, 3), ("A", 0, 1), ("G", (2, 3), 0), ("A", 1, 1),
       ("F", ((0, 0), (0, 1)), 1), ("C", 0, 0), ("C", 1, 0))


def kernel(dps, tensors, sections, hidden_ref, gain_ref, lens_ref, gate_hbm, up_hbm, down_hbm,
           out_ref, gate_v, up_v, down_v, down_t, x_in, x_parts, scaled_v, part_out, part_in, own_gu, own_ss, half_ss, inv_v,
           cross_out, cross_in, h_out, hid, acc_v, tx, outs, gram, lbuf, lens_full,
           w_sem, d_send, d_recv, x_send, x_recv, p_send, p_recv, r_send, r_recv, h_send, h_recv, t_send, t_recv,
           g_send, g_recv, l_send, l_recv):
    section = lax.axis_index("section")
    tensor = lax.axis_index("tensor")
    dp = lax.axis_index("dp")
    micros = dps * SPLIT
    width = gate_v.shape[0]
    cols = gate_v.shape[1]
    fc = cols // (2 * Q)
    rows = x_in.shape[1]
    d_model = width * dps
    half = dps // 2
    pair = 2 if tensors % 2 == 0 else 1
    lead = pair - 1
    first = tensor - lax.rem(tensor, pair)
    core = lax.rem(tensor, pair)
    side = dp // half
    hub_dp = half - 1 + side
    out_way = 2 * side - 1
    reach = (dp - hub_dp) * out_way
    is_hub = jnp.logical_and(reach == 0, core == lead)
    held = hidden_ref.shape[1]
    pw = min(held, width)
    nj = held // pw
    np_ = width // pw

    def chunk_at(which, q):
        return (side if which == 0 else 1 - side) * Q + q

    def chunk_of(j):
        return chunk_at(1, j) if j < Q else chunk_at(0, j - Q)

    def columns(c):
        return pl.ds(pl.multiple_of(c * fc, fc), fc)

    def wcopy(which, c):
        src, dst = ((gate_hbm, gate_v), (up_hbm, up_v), (down_hbm, down_v))[which]
        return pltpu.make_async_copy(src.at[0, :, columns(c)], dst.at[:, columns(c)], w_sem.at[which, c])

    for c in range(2 * Q):
        wcopy(2, c).start()
    for j in range(2 * Q):
        wcopy(0, chunk_of(j)).start()
        wcopy(1, chunk_of(j)).start()

    barrier = pltpu.get_barrier_semaphore()
    for kt in range(tensors):
        for kd in range(dps):
            if kt or kd:
                pl.semaphore_signal(
                    barrier, inc=1,
                    device_id={"tensor": lax.rem(tensor + kt, tensors), "dp": lax.rem(dp + kd, dps)},
                    device_id_type=MESH)

    @pl.when(section > 0)
    def _():
        for k in range(tensors):
            pl.semaphore_signal(barrier, inc=1, device_id={"section": section - 1, "tensor": k}, device_id_type=MESH)

    @pl.when(section < sections - 1)
    def _():
        for k in range(tensors):
            pl.semaphore_signal(barrier, inc=1, device_id={"section": section + 1, "tensor": k}, device_id_type=MESH)

    pl.semaphore_wait(
        barrier,
        tensors * dps - 1 + jnp.where(section == 0, 0, tensors) + jnp.where(section == sections - 1, 0, tensors))

    each = lens_ref.shape[0]
    sents = each * dps
    peers = [lax.rem(dp + k, dps) for k in range(1, dps)]
    slot = lax.broadcasted_iota(jnp.int32, lbuf.shape[1:], 0)
    own_lens = jnp.ones(lbuf.shape[1:], F32)
    for n in range(each):
        own_lens = jnp.where(slot == n, lens_ref[n].astype(F32), own_lens)
    lbuf[dp] = own_lens

    def s_copy(buf, send, recv, c, peer):
        return pltpu.make_async_remote_copy(
            src_ref=buf.at[c], dst_ref=buf.at[c], send_sem=send.at[peer], recv_sem=recv.at[c],
            device_id={"dp": peer}, device_id_type=MESH)

    def spread(m, j, k):
        h = lax.rem(m, SPLIT)
        at = tensor * held + j * pw
        piece = lax.rem(at, width) // pw
        return pltpu.make_async_remote_copy(
            src_ref=hidden_ref.at[pl.ds(pl.multiple_of(h * rows, rows), rows), pl.ds(j * pw, pw)],
            dst_ref=x_in.at[m, :, pl.ds(pl.multiple_of(piece * pw, pw), pw)],
            send_sem=d_send.at[h, j * tensors + k], recv_sem=d_recv.at[m, piece],
            device_id={"tensor": lax.rem(tensor + k, tensors), "dp": at // width}, device_id_type=MESH)

    def spread_all(m, act):
        @pl.when(jnp.logical_and(section == 0, m // SPLIT == dp))
        def _():
            for j in range(nj):
                at = tensor * held + j * pw
                for k in range(tensors):
                    if k:
                        act(m, j, k)
                    else:
                        @pl.when(at // width != dp)
                        def _():
                            act(m, j, k)

    def spread_start(m):
        spread_all(m, lambda m, j, k: spread(m, j, k).start())

        @pl.when(jnp.logical_and(section == 0, m // SPLIT == dp))
        def _():
            h = lax.rem(m, SPLIT)
            for j in range(nj):
                at = tensor * held + j * pw
                piece = lax.rem(at, width) // pw

                @pl.when(at // width == dp)
                def _():
                    x_in[m, :, pl.ds(pl.multiple_of(piece * pw, pw), pw)] = hidden_ref[
                        pl.ds(pl.multiple_of(h * rows, rows), rows), j * pw:(j + 1) * pw]

    def early(m, carry):
        spread_start(m)
        return carry

    lax.fori_loop(0, AHEAD, early, 0)
    for c in peers:
        s_copy(lbuf, l_send, l_recv, dp, c).start()

    def p_part(ref, j):
        return ref.at[:, pl.ds(0, 2 * fc + LANES)] if j == 0 else ref.at[:, pl.ds(0, 2 * fc)]

    def p_copy(m, j):
        at = reach * pair + core
        return pltpu.make_async_remote_copy(
            src_ref=p_part(part_out.at[m, j], j), dst_ref=p_part(part_in.at[m, at, j], j),
            send_sem=p_send.at[m, j], recv_sem=p_recv.at[m, at * 2 * Q + j],
            device_id={"dp": hub_dp, "tensor": first + lead}, device_id_type=MESH)

    def p_wait(m, at, j):
        ref = p_part(part_in.at[m, at, j], j)
        pltpu.make_async_remote_copy(
            src_ref=ref, dst_ref=ref, send_sem=p_send.at[m, j], recv_sem=p_recv.at[m, at * 2 * Q + j],
            device_id={"dp": 1 - side}, device_id_type=MESH).wait_recv()

    def r_copy(m, k, q):
        j = 0 if q == 0 and k == lead else 1
        return pltpu.make_async_remote_copy(
            src_ref=p_part(cross_out.at[m, k, q], j), dst_ref=p_part(cross_in.at[m, k, q], j),
            send_sem=r_send.at[m, k * Q + q], recv_sem=r_recv.at[m, k * Q + q],
            device_id={"dp": hub_dp - out_way}, device_id_type=MESH)

    targets = [dp - out_way * r for r in range(half, 0, -1)] + [dp + out_way * r for r in range(1, half)]

    def h_copy(m, k, q, n):
        to = {"dp": targets[n], "tensor": first + k} if n < dps - 1 else {"tensor": first + k}
        return pltpu.make_async_remote_copy(
            src_ref=h_out.at[m, k, q], dst_ref=hid.at[m, side * Q + q],
            send_sem=h_send.at[m, (k * Q + q) * dps + n], recv_sem=h_recv.at[m, side * Q + q],
            device_id=to, device_id_type=MESH)

    def h_wait(m, c):
        pltpu.make_async_remote_copy(
            src_ref=hid.at[m, c], dst_ref=hid.at[m, c], send_sem=h_send.at[m, 0], recv_sem=h_recv.at[m, c],
            device_id={"dp": 1 - side}, device_id_type=MESH).wait_recv()

    def h_sends(k):
        return range(dps - 1 if k == lead else dps)

    def t_copy(m, t, peer):
        return pltpu.make_async_remote_copy(
            src_ref=tx.at[m, t], dst_ref=tx.at[m, t],
            send_sem=t_send.at[m, peer], recv_sem=t_recv.at[m, t],
            device_id={"tensor": peer}, device_id_type=MESH)

    def x_copy(m, t, k, to):
        return pltpu.make_async_remote_copy(
            src_ref=tx.at[m, t], dst_ref=x_parts.at[m, t],
            send_sem=x_send.at[m, k], recv_sem=x_recv.at[m, t],
            device_id={"section": to, "tensor": k}, device_id_type=MESH)

    lane = lax.broadcasted_iota(jnp.int32, (rows, LANES), 1)

    def pack(ss):
        high = ss.astype(BF16)
        low = (ss - high.astype(F32)).astype(BF16)
        return jnp.where(lane < LANES // 2, high.astype(F32), low.astype(F32)).astype(BF16)

    def unpack(lanes):
        return jnp.sum(lanes.astype(F32), axis=1, keepdims=True) * (2.0 / LANES)

    def enter(m):
        @pl.when(section == 0)
        def _():
            for piece in range(np_):
                source = (dp * width + piece * pw) // held

                @pl.when(jnp.logical_not(jnp.logical_and(m // SPLIT == dp, source == tensor)))
                def _():
                    ref = x_in.at[m, :, pl.ds(piece * pw, pw)]
                    pltpu.make_async_remote_copy(
                        src_ref=ref, dst_ref=ref, send_sem=d_send.at[0, 0], recv_sem=d_recv.at[m, piece],
                        device_id={"dp": 1 - side}, device_id_type=MESH).wait_recv()

        @pl.when(section > 0)
        def _():
            total = None
            for t in range(tensors):
                x_copy(m, t, 0, 0).wait_recv()
                term = x_parts[m, t].astype(F32)
                total = term if total is None else total + term
            x_in[m] = total.astype(BF16)

        x = x_in[m].astype(F32)
        own_ss[m] = jnp.broadcast_to(jnp.sum(x * x, axis=1, keepdims=True), (rows, LANES))
        scaled_v[...] = (x * gain_ref[:, pl.ds(pl.multiple_of(dp * width, width), width)]).astype(BF16)

    def project(m, hub, js):
        @pl.when(m == 0)
        def _():
            for j in js:
                wcopy(0, chunk_of(j)).wait()
                wcopy(1, chunk_of(j)).wait()

        if js[0] == 0:
            enter(m)
        for j in js:
            c = chunk_of(j)
            g = jnp.dot(scaled_v[...], gate_v[:, columns(c)], preferred_element_type=F32)
            u = jnp.dot(scaled_v[...], up_v[:, columns(c)], preferred_element_type=F32)
            if hub:
                own_gu[m, j, :, 0:fc] = g
                own_gu[m, j, :, fc:2 * fc] = u
            else:
                part_out[m, j, :, 0:fc] = g.astype(BF16)
                part_out[m, j, :, fc:2 * fc] = u.astype(BF16)
                if j == 0:
                    part_out[m, j, :, 2 * fc:2 * fc + LANES] = pack(own_ss[m][:, 0:1])
                p_copy(m, j).start()

    def sources(k):
        return [r * pair + k for r in range(half) if r or k != lead]

    def gathered(m, k, j):
        total = own_gu[m, j] if k == lead else None
        for at in sources(k):
            term = part_in[m, at, j, :, 0:2 * fc].astype(F32)
            total = term if total is None else total + term
        return total

    def combine(m, q):
        for k in reversed(range(pair)):
            for at in sources(k):
                p_wait(m, at, q)
            cross_out[m, k, q, :, 0:2 * fc] = gathered(m, k, q).astype(BF16)
            if q == 0 and k == lead:
                ss = own_ss[m][:, 0:1]
                for at in sources(k):
                    ss = ss + unpack(part_in[m, at, 0, :, 2 * fc:2 * fc + LANES])
                half_ss[m] = jnp.broadcast_to(ss, (rows, LANES))
                cross_out[m, k, q, :, 2 * fc:2 * fc + LANES] = pack(ss)
            r_copy(m, k, q).start()

    def activate(m, q):
        for k in reversed(range(pair)):
            for at in sources(k):
                p_wait(m, at, Q + q)
            r_copy(m, k, q).wait_recv()
            if q == 0 and k == lead:
                ss = half_ss[m][:, 0:1] + unpack(cross_in[m, k, 0, :, 2 * fc:2 * fc + LANES])
                inv_v[m] = jnp.broadcast_to(lax.rsqrt(ss * (1.0 / d_model) + RMS_EPS), (rows, LANES))
            gu = (gathered(m, k, Q + q) + cross_in[m, k, q, :, 0:2 * fc].astype(F32)) * inv_v[m][:, 0:1]
            g = gu[:, 0:fc]
            made = (g / (1.0 + jnp.exp(-g)) * gu[:, fc:2 * fc]).astype(BF16)
            h_out[m, k, q] = made
            for n in h_sends(k):
                h_copy(m, k, q, n).start()
            if k == lead:
                hid[m, side * Q + q] = made

    def descend(m, hub, parts):
        acc = None if parts[0] == (0, 0) else acc_v[m]
        for which, q in parts:
            if not (hub and which == 0):
                h_wait(m, chunk_at(which, q))
        for which, q in parts:
            c = chunk_at(which, q)
            term = jnp.dot(hid[m, c], down_t[columns(c), :], preferred_element_type=F32)
            acc = term if acc is None else acc + term
        if parts[-1] != (1, Q - 1):
            acc_v[m] = acc
        else:
            tx[m, tensor] = (acc + x_in[m].astype(F32) * (1.0 / tensors)).astype(BF16)

            @pl.when(section < sections - 1)
            def _():
                for k in range(tensors):
                    x_copy(m, tensor, k, section + 1).start()

            for k in range(1, tensors):
                t_copy(m, tensor, lax.rem(tensor + k, tensors)).start()

    def settle(m):
        for k in range(1, tensors):
            other = lax.rem(tensor + k, tensors)
            t_copy(m, other, other).wait_recv()
        total = tx[m, 0].astype(F32)
        for t in range(1, tensors):
            total = total + tx[m, t].astype(F32)
        outs[m] = total.astype(BF16)

    turn = min(fc, 2 * LANES)
    for c in range(2 * Q):
        wcopy(2, c).wait()

        def flip(b, carry):
            at = pl.ds(pl.multiple_of(c * fc + b * turn, turn), turn)
            down_t[at, :] = down_v[:, at].T
            return carry

        lax.fori_loop(0, fc // turn, flip, 0)

    def run(hub):
        steps = HUB if hub else LEAF

        def step(i, carry):
            spread_next = i + AHEAD

            @pl.when(spread_next < micros)
            def _():
                spread_start(spread_next)

            for op, arg, lag in steps:
                m = i - lag

                @pl.when(jnp.logical_and(m >= 0, m < micros))
                def _():
                    if op == "G":
                        project(m, hub, arg)
                    elif op == "C":
                        combine(m, arg)
                    elif op == "A":
                        activate(m, arg)
                    elif op == "F":
                        descend(m, hub, arg)
                    else:
                        settle(m)
            return carry

        lax.fori_loop(0, micros + max(lag for _, _, lag in steps), step, 0)

    @pl.when(is_hub)
    def _():
        run(True)

        def drain(m, carry):
            for k in range(pair):
                for q in range(Q):
                    r_copy(m, k, q).wait_send()
                    for n in h_sends(k):
                        h_copy(m, k, q, n).wait_send()
            return carry

        lax.fori_loop(0, micros, drain, 0)

    @pl.when(jnp.logical_not(is_hub))
    def _():
        run(False)

        def drain(m, carry):
            for j in range(2 * Q):
                p_copy(m, j).wait_send()
            return carry

        lax.fori_loop(0, micros, drain, 0)

    for c in peers:
        s_copy(lbuf, l_send, l_recv, c, c).wait_recv()
    for c in range(dps):
        lens_full[c * each:(c + 1) * each] = lbuf[c, 0:each]
    tokens = micros * rows
    per = tokens // sents
    place = lax.broadcasted_iota(jnp.int32, (sents, tokens), 1) - per * lax.broadcasted_iota(
        jnp.int32, (sents, tokens), 0)
    lens = lens_full[:, 0:1]
    valid = jnp.logical_and(place >= 0, place.astype(F32) < lens)
    mask = jnp.where(valid, 1.0, 0.0).astype(BF16)
    pooled = jnp.dot(mask, outs[...].reshape(tokens, width), preferred_element_type=F32) / lens

    def share(buf, send, recv):
        for c in peers:
            s_copy(buf, send, recv, dp, c).start()
        for c in peers:
            s_copy(buf, send, recv, c, c).wait_recv()

    mean = jnp.sum(pooled, axis=1, keepdims=True) * (1.0 / width)
    centered = pooled - mean
    narrow = centered.astype(BF16)
    sq = jnp.sum(centered * centered, axis=1, keepdims=True)
    gram[dp, 0] = jnp.zeros((sents, LANES), F32)
    gram[dp, 0, :, 0:sents] = lax.dot_general(narrow, narrow, CONTRACT_LAST, preferred_element_type=F32)
    gram[dp, 1] = jnp.broadcast_to(sq, (sents, LANES))
    gram[dp, 2] = jnp.broadcast_to(mean, (sents, LANES))
    share(gram, g_send, g_recv)
    products, sq, mean = gram[0, 0], gram[0, 1], gram[0, 2]
    for c in range(1, dps):
        products = products + gram[c, 0]
        sq = sq + gram[c, 1]
        mean = mean + gram[c, 2]
    mean = mean * (1.0 / dps)
    r_i = lax.broadcasted_iota(jnp.int32, (sents, LANES), 0)
    c_i = lax.broadcasted_iota(jnp.int32, (sents, LANES), 1)
    for c in range(dps):
        off = gram[c, 2] - mean
        off_row = jnp.sum(jnp.where(r_i == c_i, off, 0.0), axis=0, keepdims=True)
        products = products + off * off_row * float(width)
        sq = sq + off * off * float(width)
    scale = lax.rsqrt(sq * (1.0 / d_model) + UNIT_FLOOR)
    across = jnp.sum(jnp.where(r_i == c_i, scale, 0.0), axis=0, keepdims=True)
    whole = 1.0 - products * scale * across * (1.0 / d_model)
    for r in range(each):
        row = jnp.sum(jnp.where(r_i == dp * each + r, whole, 0.0), axis=0, keepdims=True)
        out_ref[0, r:r + 1, :] = row[:, 0:sents]

    def drain(m, carry):
        spread_all(m, lambda m, j, k: spread(m, j, k).wait_send())
        for k in range(1, tensors):
            t_copy(m, tensor, lax.rem(tensor + k, tensors)).wait_send()

        @pl.when(section < sections - 1)
        def _():
            for k in range(tensors):
                x_copy(m, tensor, k, section + 1).wait_send()
        return carry

    lax.fori_loop(0, micros, drain, 0)
    for c in peers:
        s_copy(lbuf, l_send, l_recv, dp, c).wait_send()
        s_copy(gram, g_send, g_recv, dp, c).wait_send()


def per_device(hidden_in, norm_gain, gate_weight, up_weight, down_weight, lengths):
    sections = lax.axis_size("section")
    tensors = lax.axis_size("tensor")
    dps = lax.axis_size("dp")
    _, width, cols = gate_weight.shape
    micros = dps * SPLIT
    rows = hidden_in.shape[0] // SPLIT
    fc = cols // (2 * Q)
    half = dps // 2
    pair = 2 if tensors % 2 == 0 else 1
    held = hidden_in.shape[1]
    pw = min(held, width)
    each = lengths.shape[0]
    sents = each * dps
    vm = pl.BlockSpec(memory_space=pltpu.VMEM)
    hbm = pl.BlockSpec(memory_space=pl.ANY)
    dma = pltpu.SemaphoreType.DMA
    smem = pl.BlockSpec(memory_space=pltpu.SMEM)
    return pl.pallas_call(
        functools.partial(kernel, dps, tensors, sections),
        out_shape=jax.ShapeDtypeStruct((1, each, sents), F32),
        in_specs=[vm] * 2 + [smem] + [hbm] * 3,
        out_specs=vm,
        scratch_shapes=[
            pltpu.VMEM((width, cols), BF16),
            pltpu.VMEM((width, cols), BF16),
            pltpu.VMEM((width, cols), BF16),
            pltpu.VMEM((cols, width), BF16),
            pltpu.VMEM((micros, rows, width), BF16),
            pltpu.VMEM((micros, tensors, rows, width), BF16),
            pltpu.VMEM((rows, width), BF16),
            pltpu.VMEM((micros, 2 * Q, rows, 2 * fc + LANES), BF16),
            pltpu.VMEM((micros, half * pair, 2 * Q, rows, 2 * fc + LANES), BF16),
            pltpu.VMEM((micros, 2 * Q, rows, 2 * fc), F32),
            pltpu.VMEM((micros, rows, LANES), F32),
            pltpu.VMEM((micros, rows, LANES), F32),
            pltpu.VMEM((micros, rows, LANES), F32),
            pltpu.VMEM((micros, pair, Q, rows, 2 * fc + LANES), BF16),
            pltpu.VMEM((micros, pair, Q, rows, 2 * fc + LANES), BF16),
            pltpu.VMEM((micros, pair, Q, rows, fc), BF16),
            pltpu.VMEM((micros, 2 * Q, rows, fc), BF16),
            pltpu.VMEM((micros, rows, width), F32),
            pltpu.VMEM((micros, tensors, rows, width), BF16),
            pltpu.VMEM((micros, rows, width), BF16),
            pltpu.VMEM((dps, 3, sents, LANES), F32),
            pltpu.VMEM((dps, -(-each // 8) * 8, LANES), F32),
            pltpu.VMEM((sents, LANES), F32),
            dma((3, 2 * Q)),
            dma((SPLIT, held // pw * tensors)),
            dma((micros, width // pw)),
            dma((micros, tensors)),
            dma((micros, tensors)),
            dma((micros, 2 * Q)),
            dma((micros, half * pair * 2 * Q)),
            dma((micros, pair * Q)),
            dma((micros, pair * Q)),
            dma((micros, pair * Q * dps)),
            dma((micros, 2 * Q)),
            dma((micros, tensors)),
            dma((micros, tensors)),
            dma((dps,)),
            dma((dps,)),
            dma((dps,)),
            dma((dps,)),
        ],
        compiler_params=pltpu.CompilerParams(
            collective_id=0, has_side_effects=True, vmem_limit_bytes=60 * 1024 * 1024),
    )(hidden_in, norm_gain, lengths, gate_weight, up_weight, down_weight)


def solution(mesh):
    placed = (
        P("dp", "tensor"),
        P("section", None),
        P("section", "dp", "tensor"),
        P("section", "dp", "tensor"),
        P("section", "dp", "tensor"),
        P("dp"),
    )
    return jax.shard_map(
        per_device, mesh=mesh, in_specs=placed, out_specs=P("section", "dp", None), check_vma=False
    )
```

```python
import functools

import jax
import jax.numpy as jnp
from jax import lax
from jax.experimental import pallas as pl
from jax.experimental.pallas import tpu as pltpu
from jax.sharding import PartitionSpec as P

RMS_EPS = 1e-05
UNIT_FLOOR = 0.1
CONTRACT_LAST = (((1,), (1,)), ((), ()))
MESH = pl.DeviceIdType.MESH
LANES = 128
F32 = jnp.float32
BF16 = jnp.bfloat16

SPLIT = 2
Q = 2

LEAF = (("G", (0,), 0), ("F", ((0, 0), (1, 0)), 2), ("G", (1,), 0), ("F", ((0, 1), (1, 1)), 2), ("E", None, 3),
        ("G", (2, 3), 0))
HUB = (("G", (0, 1), 0), ("F", ((1, 0), (1, 1)), 2), ("A", 0, 1), ("G", (2,), 0), ("A", 1, 1), ("G", (3,), 0),
       ("C", 0, 0), ("F", ((0, 0), (0, 1)), 1), ("C", 1, 0), ("E", None, 3))


def kernel(dps, tensors, sections, hidden_ref, gain_ref, lens_ref, gate_hbm, up_hbm, down_hbm,
           out_ref, gate_v, up_v, down_v, down_t, x_in, x_parts, scaled_v, part_out, part_in, own_gu, own_ss, half_ss, inv_v,
           cross_out, cross_in, h_out, hid, acc_v, tx, outs, gram, lbuf, lens_full,
           w_sem, d_send, d_recv, x_send, x_recv, p_send, p_recv, r_send, r_recv, h_send, h_recv, t_send, t_recv,
           g_send, g_recv, l_send, l_recv):
    section = lax.axis_index("section")
    tensor = lax.axis_index("tensor")
    dp = lax.axis_index("dp")
    micros = dps * SPLIT
    width = gate_v.shape[0]
    cols = gate_v.shape[1]
    fc = cols // (2 * Q)
    rows = x_in.shape[1]
    d_model = width * dps
    half = dps // 2
    pair = 2 if tensors % 2 == 0 else 1
    lead = pair - 1
    first = tensor - lax.rem(tensor, pair)
    core = lax.rem(tensor, pair)
    side = dp // half
    hub_dp = half - 1 + side
    out_way = 2 * side - 1
    reach = (dp - hub_dp) * out_way
    is_hub = jnp.logical_and(reach == 0, core == lead)
    held = hidden_ref.shape[1]
    pw = min(held, width)
    nj = held // pw
    np_ = width // pw

    def chunk_at(which, q):
        return (side if which == 0 else 1 - side) * Q + q

    def chunk_of(j):
        return chunk_at(1, j) if j < Q else chunk_at(0, j - Q)

    def columns(c):
        return pl.ds(pl.multiple_of(c * fc, fc), fc)

    def wcopy(which, c):
        src, dst = ((gate_hbm, gate_v), (up_hbm, up_v), (down_hbm, down_v))[which]
        return pltpu.make_async_copy(src.at[0, :, columns(c)], dst.at[:, columns(c)], w_sem.at[which, c])

    for c in range(2 * Q):
        wcopy(2, c).start()
    for j in range(2 * Q):
        wcopy(0, chunk_of(j)).start()
        wcopy(1, chunk_of(j)).start()

    barrier = pltpu.get_barrier_semaphore()
    for kt in range(tensors):
        for kd in range(dps):
            if kt or kd:
                pl.semaphore_signal(
                    barrier, inc=1,
                    device_id={"tensor": lax.rem(tensor + kt, tensors), "dp": lax.rem(dp + kd, dps)},
                    device_id_type=MESH)

    @pl.when(section > 0)
    def _():
        for k in range(tensors):
            pl.semaphore_signal(barrier, inc=1, device_id={"section": section - 1, "tensor": k}, device_id_type=MESH)

    @pl.when(section < sections - 1)
    def _():
        for k in range(tensors):
            pl.semaphore_signal(barrier, inc=1, device_id={"section": section + 1, "tensor": k}, device_id_type=MESH)

    pl.semaphore_wait(
        barrier,
        tensors * dps - 1 + jnp.where(section == 0, 0, tensors) + jnp.where(section == sections - 1, 0, tensors))

    each = lens_ref.shape[0]
    sents = each * dps
    peers = [lax.rem(dp + k, dps) for k in range(1, dps)]
    slot = lax.broadcasted_iota(jnp.int32, lbuf.shape[1:], 0)
    own_lens = jnp.ones(lbuf.shape[1:], F32)
    for n in range(each):
        own_lens = jnp.where(slot == n, lens_ref[n].astype(F32), own_lens)
    lbuf[dp] = own_lens

    def s_copy(buf, send, recv, c, peer):
        return pltpu.make_async_remote_copy(
            src_ref=buf.at[c], dst_ref=buf.at[c], send_sem=send.at[peer], recv_sem=recv.at[c],
            device_id={"dp": peer}, device_id_type=MESH)

    def spread(m, j, k):
        h = lax.rem(m, SPLIT)
        at = tensor * held + j * pw
        piece = lax.rem(at, width) // pw
        return pltpu.make_async_remote_copy(
            src_ref=hidden_ref.at[pl.ds(pl.multiple_of(h * rows, rows), rows), pl.ds(j * pw, pw)],
            dst_ref=x_in.at[m, :, pl.ds(pl.multiple_of(piece * pw, pw), pw)],
            send_sem=d_send.at[h, j * tensors + k], recv_sem=d_recv.at[m, piece],
            device_id={"tensor": lax.rem(tensor + k, tensors), "dp": at // width}, device_id_type=MESH)

    def spread_all(m, act):
        @pl.when(jnp.logical_and(section == 0, m // SPLIT == dp))
        def _():
            for j in range(nj):
                at = tensor * held + j * pw
                for k in range(tensors):
                    if k:
                        act(m, j, k)
                    else:
                        @pl.when(at // width != dp)
                        def _():
                            act(m, j, k)

    def spread_start(m):
        spread_all(m, lambda m, j, k: spread(m, j, k).start())

        @pl.when(jnp.logical_and(section == 0, m // SPLIT == dp))
        def _():
            h = lax.rem(m, SPLIT)
            for j in range(nj):
                at = tensor * held + j * pw
                piece = lax.rem(at, width) // pw

                @pl.when(at // width == dp)
                def _():
                    x_in[m, :, pl.ds(pl.multiple_of(piece * pw, pw), pw)] = hidden_ref[
                        pl.ds(pl.multiple_of(h * rows, rows), rows), j * pw:(j + 1) * pw]

    def early(m, carry):
        spread_start(m)
        return carry

    lax.fori_loop(0, micros, early, 0)

    def p_part(ref, j):
        return ref.at[:, pl.ds(0, 2 * fc + LANES)] if j == 0 else ref.at[:, pl.ds(0, 2 * fc)]

    def p_copy(m, j):
        at = reach * pair + core
        return pltpu.make_async_remote_copy(
            src_ref=p_part(part_out.at[m, j], j), dst_ref=p_part(part_in.at[m, at, j], j),
            send_sem=p_send.at[m, j], recv_sem=p_recv.at[m, at * 2 * Q + j],
            device_id={"dp": hub_dp, "tensor": first + lead}, device_id_type=MESH)

    def p_wait(m, at, j):
        ref = p_part(part_in.at[m, at, j], j)
        pltpu.make_async_remote_copy(
            src_ref=ref, dst_ref=ref, send_sem=p_send.at[m, j], recv_sem=p_recv.at[m, at * 2 * Q + j],
            device_id={"dp": 1 - side}, device_id_type=MESH).wait_recv()

    def r_copy(m, k, q):
        j = 0 if q == 0 and k == lead else 1
        return pltpu.make_async_remote_copy(
            src_ref=p_part(cross_out.at[m, k, q], j), dst_ref=p_part(cross_in.at[m, k, q], j),
            send_sem=r_send.at[m, k * Q + q], recv_sem=r_recv.at[m, k * Q + q],
            device_id={"dp": hub_dp - out_way}, device_id_type=MESH)

    targets = [dp - out_way * r for r in range(half, 0, -1)] + [dp + out_way * r for r in range(1, half)]

    def h_copy(m, k, q, n):
        to = {"dp": targets[n], "tensor": first + k} if n < dps - 1 else {"tensor": first + k}
        return pltpu.make_async_remote_copy(
            src_ref=h_out.at[m, k, q], dst_ref=hid.at[m, side * Q + q],
            send_sem=h_send.at[m, (k * Q + q) * dps + n], recv_sem=h_recv.at[m, side * Q + q],
            device_id=to, device_id_type=MESH)

    def h_wait(m, c):
        pltpu.make_async_remote_copy(
            src_ref=hid.at[m, c], dst_ref=hid.at[m, c], send_sem=h_send.at[m, 0], recv_sem=h_recv.at[m, c],
            device_id={"dp": 1 - side}, device_id_type=MESH).wait_recv()

    def h_sends(k):
        return range(dps - 1 if k == lead else dps)

    def t_copy(m, t, peer):
        return pltpu.make_async_remote_copy(
            src_ref=tx.at[m, t], dst_ref=tx.at[m, t],
            send_sem=t_send.at[m, peer], recv_sem=t_recv.at[m, t],
            device_id={"tensor": peer}, device_id_type=MESH)

    def x_copy(m, t, k, to):
        return pltpu.make_async_remote_copy(
            src_ref=tx.at[m, t], dst_ref=x_parts.at[m, t],
            send_sem=x_send.at[m, k], recv_sem=x_recv.at[m, t],
            device_id={"section": to, "tensor": k}, device_id_type=MESH)

    lane = lax.broadcasted_iota(jnp.int32, (rows, LANES), 1)

    def pack(ss):
        high = ss.astype(BF16)
        low = (ss - high.astype(F32)).astype(BF16)
        return jnp.where(lane < LANES // 2, high.astype(F32), low.astype(F32)).astype(BF16)

    def unpack(lanes):
        return jnp.sum(lanes.astype(F32), axis=1, keepdims=True) * (2.0 / LANES)

    def enter(m):
        @pl.when(section == 0)
        def _():
            for piece in range(np_):
                source = (dp * width + piece * pw) // held

                @pl.when(jnp.logical_not(jnp.logical_and(m // SPLIT == dp, source == tensor)))
                def _():
                    ref = x_in.at[m, :, pl.ds(piece * pw, pw)]
                    pltpu.make_async_remote_copy(
                        src_ref=ref, dst_ref=ref, send_sem=d_send.at[0, 0], recv_sem=d_recv.at[m, piece],
                        device_id={"dp": 1 - side}, device_id_type=MESH).wait_recv()

        @pl.when(section > 0)
        def _():
            total = None
            for t in range(tensors):
                x_copy(m, t, 0, 0).wait_recv()
                term = x_parts[m, t].astype(F32)
                total = term if total is None else total + term
            x_in[m] = total.astype(BF16)

        x = x_in[m].astype(F32)
        own_ss[m] = jnp.broadcast_to(jnp.sum(x * x, axis=1, keepdims=True), (rows, LANES))
        scaled_v[...] = (x * gain_ref[:, pl.ds(pl.multiple_of(dp * width, width), width)]).astype(BF16)

    def project(m, hub, js):
        @pl.when(m == 0)
        def _():
            for j in js:
                wcopy(0, chunk_of(j)).wait()
                wcopy(1, chunk_of(j)).wait()

        if js[0] == 0:
            enter(m)
        for j in js:
            c = chunk_of(j)
            g = jnp.dot(scaled_v[...], gate_v[:, columns(c)], preferred_element_type=F32)
            u = jnp.dot(scaled_v[...], up_v[:, columns(c)], preferred_element_type=F32)
            if hub:
                own_gu[m, j, :, 0:fc] = g
                own_gu[m, j, :, fc:2 * fc] = u
            else:
                part_out[m, j, :, 0:fc] = g.astype(BF16)
                part_out[m, j, :, fc:2 * fc] = u.astype(BF16)
                if j == 0:
                    part_out[m, j, :, 2 * fc:2 * fc + LANES] = pack(own_ss[m][:, 0:1])
                p_copy(m, j).start()

    def sources(k):
        return [r * pair + k for r in range(half) if r or k != lead]

    def gathered(m, k, j):
        total = own_gu[m, j] if k == lead else None
        for at in sources(k):
            term = part_in[m, at, j, :, 0:2 * fc].astype(F32)
            total = term if total is None else total + term
        return total

    def combine(m, q):
        for k in reversed(range(pair)):
            for at in sources(k):
                p_wait(m, at, q)
            cross_out[m, k, q, :, 0:2 * fc] = gathered(m, k, q).astype(BF16)
            if q == 0 and k == lead:
                ss = own_ss[m][:, 0:1]
                for at in sources(k):
                    ss = ss + unpack(part_in[m, at, 0, :, 2 * fc:2 * fc + LANES])
                half_ss[m] = jnp.broadcast_to(ss, (rows, LANES))
                cross_out[m, k, q, :, 2 * fc:2 * fc + LANES] = pack(ss)
            r_copy(m, k, q).start()

    def activate(m, q):
        for k in reversed(range(pair)):
            for at in sources(k):
                p_wait(m, at, Q + q)
            r_copy(m, k, q).wait_recv()
            if q == 0 and k == lead:
                ss = half_ss[m][:, 0:1] + unpack(cross_in[m, k, 0, :, 2 * fc:2 * fc + LANES])
                inv_v[m] = jnp.broadcast_to(lax.rsqrt(ss * (1.0 / d_model) + RMS_EPS), (rows, LANES))
            gu = (gathered(m, k, Q + q) + cross_in[m, k, q, :, 0:2 * fc].astype(F32)) * inv_v[m][:, 0:1]
            g = gu[:, 0:fc]
            made = (g / (1.0 + jnp.exp(-g)) * gu[:, fc:2 * fc]).astype(BF16)
            h_out[m, k, q] = made
            for n in h_sends(k):
                h_copy(m, k, q, n).start()
            if k == lead:
                hid[m, side * Q + q] = made

    def descend(m, hub, parts):
        acc = None if parts[0] == (0, 0) else acc_v[m]
        for which, q in parts:
            if not (hub and which == 0):
                h_wait(m, chunk_at(which, q))
        for which, q in parts:
            c = chunk_at(which, q)
            term = jnp.dot(hid[m, c], down_t[columns(c), :], preferred_element_type=F32)
            acc = term if acc is None else acc + term
        if parts[-1] != (1, Q - 1):
            acc_v[m] = acc
        else:
            tx[m, tensor] = (acc + x_in[m].astype(F32) * (1.0 / tensors)).astype(BF16)

            @pl.when(section < sections - 1)
            def _():
                for k in range(tensors):
                    x_copy(m, tensor, k, section + 1).start()

            for k in range(1, tensors):
                t_copy(m, tensor, lax.rem(tensor + k, tensors)).start()

    def settle(m):
        for k in range(1, tensors):
            other = lax.rem(tensor + k, tensors)
            t_copy(m, other, other).wait_recv()
        total = tx[m, 0].astype(F32)
        for t in range(1, tensors):
            total = total + tx[m, t].astype(F32)
        outs[m] = total.astype(BF16)

    turn = min(fc, 2 * LANES)
    for c in range(2 * Q):
        wcopy(2, c).wait()

        def flip(b, carry):
            at = pl.ds(pl.multiple_of(c * fc + b * turn, turn), turn)
            down_t[at, :] = down_v[:, at].T
            return carry

        lax.fori_loop(0, fc // turn, flip, 0)

    for c in peers:
        s_copy(lbuf, l_send, l_recv, dp, c).start()

    def run(hub):
        steps = HUB if hub else LEAF

        def step(i, carry):
            for op, arg, lag in steps:
                m = i - lag

                @pl.when(jnp.logical_and(m >= 0, m < micros))
                def _():
                    if op == "G":
                        project(m, hub, arg)
                    elif op == "C":
                        combine(m, arg)
                    elif op == "A":
                        activate(m, arg)
                    elif op == "F":
                        descend(m, hub, arg)
                    else:
                        settle(m)
            return carry

        lax.fori_loop(0, micros + max(lag for _, _, lag in steps), step, 0)

    @pl.when(is_hub)
    def _():
        run(True)

        def drain(m, carry):
            for k in range(pair):
                for q in range(Q):
                    r_copy(m, k, q).wait_send()
                    for n in h_sends(k):
                        h_copy(m, k, q, n).wait_send()
            return carry

        lax.fori_loop(0, micros, drain, 0)

    @pl.when(jnp.logical_not(is_hub))
    def _():
        run(False)

        def drain(m, carry):
            for j in range(2 * Q):
                p_copy(m, j).wait_send()
            return carry

        lax.fori_loop(0, micros, drain, 0)

    for c in peers:
        s_copy(lbuf, l_send, l_recv, c, c).wait_recv()
    for c in range(dps):
        lens_full[c * each:(c + 1) * each] = lbuf[c, 0:each]
    tokens = micros * rows
    per = tokens // sents
    place = lax.broadcasted_iota(jnp.int32, (sents, tokens), 1) - per * lax.broadcasted_iota(
        jnp.int32, (sents, tokens), 0)
    lens = lens_full[:, 0:1]
    valid = jnp.logical_and(place >= 0, place.astype(F32) < lens)
    mask = jnp.where(valid, 1.0, 0.0).astype(BF16)
    pooled = jnp.dot(mask, outs[...].reshape(tokens, width), preferred_element_type=F32) / lens

    def share(buf, send, recv):
        for c in peers:
            s_copy(buf, send, recv, dp, c).start()
        for c in peers:
            s_copy(buf, send, recv, c, c).wait_recv()

    mean = jnp.sum(pooled, axis=1, keepdims=True) * (1.0 / width)
    centered = pooled - mean
    narrow = centered.astype(BF16)
    sq = jnp.sum(centered * centered, axis=1, keepdims=True)
    column = lax.broadcasted_iota(jnp.int32, (sents, LANES), 1)
    gram[dp] = jnp.where(column == sents, sq, jnp.where(column == sents + 1, mean, 0.0))
    gram[dp, :, 0:sents] = lax.dot_general(narrow, narrow, CONTRACT_LAST, preferred_element_type=F32)
    share(gram, g_send, g_recv)
    products = gram[0]
    for c in range(1, dps):
        products = products + gram[c]
    sq = products[:, sents:sents + 1]
    mean = products[:, sents + 1:sents + 2] * (1.0 / dps)
    r_i = lax.broadcasted_iota(jnp.int32, (sents, LANES), 0)
    c_i = lax.broadcasted_iota(jnp.int32, (sents, LANES), 1)
    for c in range(dps):
        off = gram[c, :, sents + 1:sents + 2] - mean
        off_row = jnp.sum(jnp.where(r_i == c_i, off, 0.0), axis=0, keepdims=True)
        products = products + off * off_row * float(width)
        sq = sq + off * off * float(width)
    scale = lax.rsqrt(sq * (1.0 / d_model) + UNIT_FLOOR)
    across = jnp.sum(jnp.where(r_i == c_i, scale, 0.0), axis=0, keepdims=True)
    whole = 1.0 - products * scale * across * (1.0 / d_model)
    for r in range(each):
        row = jnp.sum(jnp.where(r_i == dp * each + r, whole, 0.0), axis=0, keepdims=True)
        out_ref[0, r:r + 1, :] = row[:, 0:sents]

    def drain(m, carry):
        spread_all(m, lambda m, j, k: spread(m, j, k).wait_send())
        for k in range(1, tensors):
            t_copy(m, tensor, lax.rem(tensor + k, tensors)).wait_send()

        @pl.when(section < sections - 1)
        def _():
            for k in range(tensors):
                x_copy(m, tensor, k, section + 1).wait_send()
        return carry

    lax.fori_loop(0, micros, drain, 0)
    for c in peers:
        s_copy(lbuf, l_send, l_recv, dp, c).wait_send()
        s_copy(gram, g_send, g_recv, dp, c).wait_send()


def per_device(hidden_in, norm_gain, gate_weight, up_weight, down_weight, lengths):
    sections = lax.axis_size("section")
    tensors = lax.axis_size("tensor")
    dps = lax.axis_size("dp")
    _, width, cols = gate_weight.shape
    micros = dps * SPLIT
    rows = hidden_in.shape[0] // SPLIT
    fc = cols // (2 * Q)
    half = dps // 2
    pair = 2 if tensors % 2 == 0 else 1
    held = hidden_in.shape[1]
    pw = min(held, width)
    each = lengths.shape[0]
    sents = each * dps
    vm = pl.BlockSpec(memory_space=pltpu.VMEM)
    hbm = pl.BlockSpec(memory_space=pl.ANY)
    dma = pltpu.SemaphoreType.DMA
    smem = pl.BlockSpec(memory_space=pltpu.SMEM)
    return pl.pallas_call(
        functools.partial(kernel, dps, tensors, sections),
        out_shape=jax.ShapeDtypeStruct((1, each, sents), F32),
        in_specs=[vm] * 2 + [smem] + [hbm] * 3,
        out_specs=vm,
        scratch_shapes=[
            pltpu.VMEM((width, cols), BF16),
            pltpu.VMEM((width, cols), BF16),
            pltpu.VMEM((width, cols), BF16),
            pltpu.VMEM((cols, width), BF16),
            pltpu.VMEM((micros, rows, width), BF16),
            pltpu.VMEM((micros, tensors, rows, width), BF16),
            pltpu.VMEM((rows, width), BF16),
            pltpu.VMEM((micros, 2 * Q, rows, 2 * fc + LANES), BF16),
            pltpu.VMEM((micros, half * pair, 2 * Q, rows, 2 * fc + LANES), BF16),
            pltpu.VMEM((micros, 2 * Q, rows, 2 * fc), F32),
            pltpu.VMEM((micros, rows, LANES), F32),
            pltpu.VMEM((micros, rows, LANES), F32),
            pltpu.VMEM((micros, rows, LANES), F32),
            pltpu.VMEM((micros, pair, Q, rows, 2 * fc + LANES), BF16),
            pltpu.VMEM((micros, pair, Q, rows, 2 * fc + LANES), BF16),
            pltpu.VMEM((micros, pair, Q, rows, fc), BF16),
            pltpu.VMEM((micros, 2 * Q, rows, fc), BF16),
            pltpu.VMEM((micros, rows, width), F32),
            pltpu.VMEM((micros, tensors, rows, width), BF16),
            pltpu.VMEM((micros, rows, width), BF16),
            pltpu.VMEM((dps, sents, LANES), F32),
            pltpu.VMEM((dps, -(-each // 8) * 8, LANES), F32),
            pltpu.VMEM((sents, LANES), F32),
            dma((3, 2 * Q)),
            dma((SPLIT, held // pw * tensors)),
            dma((micros, width // pw)),
            dma((micros, tensors)),
            dma((micros, tensors)),
            dma((micros, 2 * Q)),
            dma((micros, half * pair * 2 * Q)),
            dma((micros, pair * Q)),
            dma((micros, pair * Q)),
            dma((micros, pair * Q * dps)),
            dma((micros, 2 * Q)),
            dma((micros, tensors)),
            dma((micros, tensors)),
            dma((dps,)),
            dma((dps,)),
            dma((dps,)),
            dma((dps,)),
        ],
        compiler_params=pltpu.CompilerParams(
            collective_id=0, has_side_effects=True, vmem_limit_bytes=60 * 1024 * 1024),
    )(hidden_in, norm_gain, lengths, gate_weight, up_weight, down_weight)


def solution(mesh):
    placed = (
        P("dp", "tensor"),
        P("section", None),
        P("section", "dp", "tensor"),
        P("section", "dp", "tensor"),
        P("section", "dp", "tensor"),
        P("dp"),
    )
    return jax.shard_map(
        per_device, mesh=mesh, in_specs=placed, out_specs=P("section", "dp", None), check_vma=False
    )
```
